32 devices in a mesh: sx: 8 (over z, y), sy: 4 (over x, core).
Axes of the slice: x: 2, y: 2, z: 4, core: 2. Of those that a mesh axis runs over, the one named last changes fastest.
Arguments:
- tensors: bfloat16 [2, 8, 4, 1024, 256], P(None, 'sx', 'sy'), may hold values from -6 to 6
- gates: bfloat16 [5, 2, 2, 256, 256], replicated, may hold values from -0.1875 to 0.1875
- closing_rows: bfloat16 [2, 4096, 1024], P(None, ('sx', 'sy')), may hold values from -0.125 to 0.125
- closing_columns: float32 [2, 4096, 256], P(None, ('sx', 'sy')), may hold values from -0.25 to 0.25
Outputs:
- amplitudes: float32 [2, 4096], replicated
The draws below stay inside these ranges and needn't reach their ends.
All inputs are finite; a program needn't handle non-finite values.
Results may differ from the reference program's by a relative error of at most 0.012.
Values may be sent and summed in bfloat16 or wider, within the bound.
A program may use at most 64 MiB of HBM per device.

```python
import jax
import jax.numpy as jnp
from jax import lax

C = 256
R = 1024
AMPS = 4096
BX = 3
SECTIONS = 5
AMP_DEV = 128
N_SX = 8
N_SY = 4


def shard_levels(stream_key, dims, pieces, smallest, largest):
    factor_of = 1.0
    for position, parts in pieces:
        heights = jax.random.uniform(jax.random.fold_in(jax.random.fold_in(stream_key, 6), position), (parts,), jnp.float32, smallest / len(pieces), largest / len(pieces))
        factor_of = factor_of * jnp.repeat(jnp.exp(heights), dims[position] // parts).reshape((-1,) + (1,) * (len(dims) - 1 - position))
    return factor_of


def scatter_about(stream_key, shape, deviation, limit, cuts=(), dtype=jnp.bfloat16):
    level = shard_levels(stream_key, shape, cuts, -0.22, 0.18) if cuts else 1.0
    entries = jax.random.normal(stream_key, shape, jnp.float32) * deviation * level
    return jnp.minimum(jnp.maximum(entries, -limit), limit).astype(dtype)


def setup_inputs(seed: int = 0) -> dict:
    key_of = jax.random.split(jax.random.key(seed), 5)
    return {
        "tensors": scatter_about(key_of[0], (2, N_SX, N_SY, R, C), 1.0, 6.0, ((1, 8), (2, 4))),
        "gates": scatter_about(key_of[1], (SECTIONS, 2, 2, C, C), (4 * C) ** -0.5, 0.1875),
        "closing_rows": scatter_about(key_of[2], (2, AMPS, R), (2 * R) ** -0.5, 0.125, ((1, 32),)),
        "closing_columns": scatter_about(key_of[3], (2, AMPS, C), (2 * C) ** -0.5, 0.25, ((1, 32),), jnp.float32),
    }


HIGH = lax.Precision.HIGHEST


def complex_product(values, matrix):
    values = values.astype(jnp.float32)
    matrix = matrix.astype(jnp.float32)
    real_part = jnp.matmul(values[0], matrix[0], precision=HIGH) - jnp.matmul(values[1], matrix[1], precision=HIGH)
    imag_part = jnp.matmul(values[0], matrix[1], precision=HIGH) + jnp.matmul(values[1], matrix[0], precision=HIGH)
    return jnp.stack([real_part, imag_part])


def apply_section(current, gate_pair, axis_dim, bit_pos):
    shape = current.shape
    count = shape[axis_dim]
    split = shape[:axis_dim] + (count >> (bit_pos + 1), 2, 1 << bit_pos) + shape[axis_dim + 1:]
    blocks = current.reshape(split)
    lower = jnp.take(blocks, 0, axis=axis_dim + 1)
    upper = jnp.take(blocks, 1, axis=axis_dim + 1)
    new_lower = complex_product(lower, gate_pair[0]) + complex_product(upper, gate_pair[1])
    new_upper = complex_product(upper, gate_pair[0]) - complex_product(lower, gate_pair[1])
    joined = jnp.stack([new_lower, new_upper], axis=axis_dim + 1).reshape(shape)
    return joined.astype(jnp.bfloat16)


def reference(tensors, gates, closing_rows, closing_columns):
    current = tensors
    for number in range(SECTIONS):
        if number < BX:
            current = apply_section(current, gates[number], 1, number)
        else:
            current = apply_section(current, gates[number], 2, number - BX)
    slices = N_SX * N_SY
    flat = current.reshape(2, slices, R, C).astype(jnp.float32)
    row_close = closing_rows.reshape(2, slices, AMP_DEV, R).astype(jnp.float32)
    column_close = closing_columns.reshape(2, slices, AMP_DEV, C)
    proj_real = jnp.matmul(row_close[0], flat[0], precision=HIGH) - jnp.matmul(row_close[1], flat[1], precision=HIGH)
    proj_imag = jnp.matmul(row_close[0], flat[1], precision=HIGH) + jnp.matmul(row_close[1], flat[0], precision=HIGH)
    amp_real = jnp.sum(proj_real * column_close[0] - proj_imag * column_close[1], axis=-1)
    amp_imag = jnp.sum(proj_real * column_close[1] + proj_imag * column_close[0], axis=-1)
    return jnp.stack([amp_real, amp_imag]).reshape(2, AMPS)
```

```python
import functools

import jax
import jax.numpy as jnp
from jax import lax
from jax.experimental import pallas as pl
from jax.experimental.pallas import tpu as pltpu
from jax.sharding import PartitionSpec as P

MESH = pl.DeviceIdType.MESH
V, O, I = 0, 1, 2
INNER, OUTER = 0, 1
Y, Z, R, G, S, U, C, F = range(8)
FIRST = (
    (U, O), (U, I), (Y, 0), (Y, 1), (Y, 2), (Y, 3), (Y, 4), (R, 0), (R, 1), (F, V), (F, O),
    (R, 3), (R, 4), (R, 2),
)
ORDERS = (
    (
        (S, 0, 0, V), (U, 0, 0), (G, 1, 0, O), (G, 0, 3, V), (Y, 0, 0), (S, 0, 3, V),
        (G, 0, 1, V), (F,), (Y, 0, 1), (S, 0, 1, V), (U, 0, 1), (G, 0, 1, O), (G, 1, 0, I),
        (G, 1, 3, O), (G, 0, 3, O), (Y, 0, 2), (S, 1, 0, I), (R, 0), (Y, 0, 3), (G, 0, 2, V),
        (G, 0, 1, I), (R, 1), (Y, 0, 4), (G, 1, 1, O), (S, 0, 2, V), (U, 0, 2), (G, 0, 3, I),
        (G, 1, 0, V), (Y, 1, 0), (S, 0, 0, I), (S, 0, 1, I), (U, 0, 3), (G, 0, 2, O), (R, 3),
        (Y, 1, 1), (Z, 0, 1), (R, 4), (S, 0, 3, I), (S, 1, 0, V), (U, 1, 0), (Z, 0, 2),
        (G, 1, 3, I), (Y, 1, 3), (R, 2), (Z, 0, 0), (C, 0, 0, 0), (C, 1, 0, 0), (Y, 1, 4),
        (C, 0, 1, 0), (C, 0, 3, 0), (G, 0, 2, I), (G, 1, 3, V), (G, 1, 1, I), (S, 0, 2, I),
        (C, 0, 2, 0), (Y, 1, 2), (S, 1, 3, V), (U, 1, 3), (G, 1, 1, V), (S, 1, 1, I),
        (Z, 1, 0), (G, 1, 2, O), (S, 1, 3, I), (C, 1, 3, 0), (S, 1, 1, V), (U, 1, 1),
        (C, 1, 1, 0), (G, 1, 2, V), (Z, 1, 1), (C, 0, 0, 1), (C, 0, 1, 1), (C, 1, 1, 1),
        (C, 1, 3, 1), (C, 0, 2, 1), (C, 1, 0, 1), (G, 1, 2, I), (S, 1, 2, V), (U, 1, 2),
        (Z, 1, 2), (C, 0, 1, 2), (C, 0, 2, 2), (C, 0, 3, 2), (C, 1, 1, 2), (C, 1, 3, 2),
        (C, 1, 0, 2), (S, 1, 2, I), (C, 1, 2, 1), (C, 1, 2, 2), (C, 1, 2, 0), (C, 0, 0, 2),
        (C, 0, 3, 1),
    ),
    (
        (F,), (S, 0, 0, O), (S, 0, 0, V), (U, 0, 0), (G, 0, 1, V), (G, 1, 0, O), (Y, 0, 0),
        (S, 1, 0, O), (G, 0, 1, O), (S, 0, 1, V), (U, 0, 1), (S, 0, 1, O), (Y, 0, 1),
        (G, 1, 1, O), (Y, 0, 2), (G, 1, 0, I), (R, 0), (G, 0, 2, V), (S, 0, 2, V), (U, 0, 2),
        (G, 1, 2, O), (R, 1), (Y, 0, 4), (S, 1, 2, O), (Y, 0, 3), (G, 0, 2, O), (G, 1, 0, V),
        (Y, 1, 0), (S, 1, 0, V), (S, 0, 2, O), (U, 1, 0), (R, 3), (Y, 1, 1), (R, 4),
        (G, 0, 3, V), (Z, 0, 3), (S, 0, 3, V), (U, 0, 3), (Y, 1, 3), (R, 2), (Z, 0, 4),
        (C, 0, 0, 0), (C, 0, 1, 0), (C, 0, 2, 0), (G, 0, 3, O), (C, 1, 0, 0), (Y, 1, 4),
        (S, 0, 3, O), (C, 0, 3, 0), (G, 1, 1, V), (S, 1, 1, V), (Y, 1, 2), (U, 1, 1),
        (G, 1, 2, V), (Z, 1, 3), (Z, 1, 4), (C, 0, 1, 1), (C, 0, 3, 1), (C, 0, 0, 1),
        (S, 1, 2, V), (U, 1, 2), (G, 1, 3, V), (C, 1, 2, 1), (C, 1, 2, 0), (G, 1, 3, O),
        (S, 1, 1, O), (C, 1, 1, 1), (C, 0, 2, 1), (C, 1, 0, 1), (C, 1, 1, 0), (S, 1, 3, V),
        (U, 1, 3), (S, 1, 3, O), (C, 1, 3, 1), (C, 1, 3, 0),
    ),
)


def outer_rows(half):
    return max(16, half * 11 // 32 // 16 * 16)


def cut(start, size, pieces):
    units = size // 16
    marks = [start + 16 * (units * k // pieces) for k in range(pieces)] + [start + size]
    return [(marks[k], marks[k + 1] - marks[k]) for k in range(pieces) if marks[k + 1] > marks[k]]


def row_chunks(half):
    low = outer_rows(half)
    return [(INNER, *span) for span in cut(low, half - low, 3)] + [
        (OUTER, *span) for span in cut(0, low, 2)
    ]


def kernel(
    plan,
    x_hbm,
    g_hbm,
    u_hbm,
    v_hbm,
    out_ref,
    xa,
    xo,
    yr,
    zr,
    x2,
    uraw,
    uo,
    ub,
    vraw,
    vb,
    gates,
    mix,
    mixz,
    back,
    wb,
    part,
    red,
    every,
    local_sem,
    send_sem,
    xrecv,
    yrecv,
    zrecv,
    grecv,
    meet_sem,
):
    exchanges, low_bit, high_bit, split_bit, gathers = plan
    half, width2 = xo.shape
    width = width2 // 2
    amps = vb.shape[2]
    slots = vb.shape[0]
    groups = slots // 8
    stages = len(exchanges)
    chunks = row_chunks(half)
    low = outer_rows(half)
    coords = {"sx": lax.axis_index("sx"), "sy": lax.axis_index("sy")}

    def bit_of(bit):
        return (coords[bit[0]] // (1 << bit[1])) % 2

    def far(*flips):
        where = dict(coords)
        for bit in flips:
            where[bit[0]] = where[bit[0]] + (1 << bit[1]) * (1 - 2 * bit_of(bit))
        return (where["sx"], where["sy"])

    is_inner = bit_of(low_bit) != bit_of(high_bit)
    mine = bit_of(split_bit)
    own_rows = pl.ds(pl.multiple_of(mine * half, half), half)
    other_rows = pl.ds(pl.multiple_of((1 - mine) * half, half), half)

    def load(src, dst, index):
        copy = pltpu.make_async_copy(src, dst, local_sem.at[index])
        copy.start()
        return copy

    v_load = load(v_hbm, vraw, 0)
    u_loads = [
        load(u_hbm.at[:, :, own_rows], uraw.at[0], 1),
        load(u_hbm.at[:, :, other_rows], uraw.at[1], 2),
    ]
    for piece in range(2):
        lanes = pl.ds(piece * width, width)
        load(x_hbm.at[piece, own_rows], xa.at[0, 0, :, lanes], 3)
        load(x_hbm.at[piece, other_rows], xo.at[:, lanes], 4)
    g_load = load(g_hbm, gates, 5)

    barrier = pltpu.get_barrier_semaphore()
    peers = [bit for bit, _ in exchanges] + [low_bit, split_bit] + [bit for bit, _ in gathers]
    for bit in peers:
        pl.semaphore_signal(barrier, inc=1, device_id=far(bit), device_id_type=MESH)

    @pl.when(is_inner)
    def _():
        pl.semaphore_signal(barrier, inc=1, device_id=far(low_bit, high_bit), device_id_type=MESH)

    v_load.wait()
    for piece in range(2):
        vb[0, pl.ds(piece * width, width)] = vraw[piece].T.astype(jnp.bfloat16)
    for index in (1, 0):
        u_loads[index].wait()
        for piece in range(2):
            lanes = pl.ds(piece * amps, amps)
            if index:
                uo[:, lanes] = uraw[1, piece].T
            else:
                ub[0, :, lanes] = uraw[0, piece].T
    pltpu.make_async_copy(xa.at[0, 0], xa.at[0, 0], local_sem.at[3]).wait()
    pltpu.make_async_copy(xo, xo, local_sem.at[4]).wait()

    @pl.when(is_inner)
    def _():
        pl.semaphore_wait(barrier, len(peers) + 1)

    @pl.when(jnp.logical_not(is_inner))
    def _():
        pl.semaphore_wait(barrier, len(peers))

    def slot_of(group, side, place):
        return group * 8 + side * 4 + place

    def area(slot, piece):
        if piece == V:
            return vb.at[slot]
        if piece == O:
            return ub.at[slot, pl.ds(0, low)]
        return ub.at[slot, pl.ds(low, half - low)]

    LOW, ACROSS, SPLIT, GATHER = 0, 1, 2, 3
    SEND_X, SEND_U, SEND_Z, SEND_V, SEND_SHARED, SEND_O, SEND_I, SEND_Y = range(8)

    def landing_sem(role, slot, piece):
        if piece == V:
            return grecv.at[slot - 1]
        if piece == (I if role == INNER else O):
            return grecv.at[slots - 1 + slot - 1]
        return grecv.at[2 * (slots - 1) + slot - 1]

    def hop_device(hop):
        if hop == LOW:
            return far(low_bit)
        if hop == ACROSS:
            return far(low_bit, high_bit)
        if hop == SPLIT:
            return far(split_bit)
        return far(gathers[hop - GATHER][0])

    def slot_copy(role, hop, source, landing, piece, src=None):
        if src is not None:
            sender = SEND_U
        elif piece == V:
            sender = SEND_V if hop < GATHER else SEND_SHARED
        else:
            sender = SEND_O if piece == O else SEND_I
        return pltpu.make_async_remote_copy(
            src_ref=area(source, piece) if src is None else src,
            dst_ref=area(landing, piece),
            send_sem=send_sem.at[sender],
            recv_sem=landing_sem(1 - role if hop == LOW else role, landing, piece),
            device_id=hop_device(hop),
            device_id_type=MESH,
        )

    def x_copy(chunk):
        here = pl.ds(*chunks[chunk][1:])
        return pltpu.make_async_remote_copy(
            src_ref=xo.at[here],
            dst_ref=xa.at[0, 1, here],
            send_sem=send_sem.at[SEND_X],
            recv_sem=xrecv.at[chunk],
            device_id=far(split_bit),
            device_id_type=MESH,
        )

    def y_copy(stage, side, chunk):
        here = pl.ds(*chunks[chunk][1:])
        return pltpu.make_async_remote_copy(
            src_ref=xa.at[stage, side, here],
            dst_ref=yr.at[stage, side, here],
            send_sem=send_sem.at[SEND_Y + stage],
            recv_sem=yrecv.at[stage, side, chunk],
            device_id=far(exchanges[stage][0]),
            device_id_type=MESH,
        )

    def z_copy(side, chunk):
        here = pl.ds(*chunks[chunk][1:])
        return pltpu.make_async_remote_copy(
            src_ref=xa.at[stages, side, here],
            dst_ref=zr.at[side, here],
            send_sem=send_sem.at[SEND_Z],
            recv_sem=zrecv.at[side, chunk],
            device_id=far(low_bit),
            device_id_type=MESH,
        )

    def scaled(value, sign):
        return value * sign.astype(jnp.float32).astype(jnp.bfloat16)

    def build_mix():
        for stage, (bit, number) in enumerate(exchanges):
            for part_ in range(2):
                real, imag = gates[number, part_, 0], gates[number, part_, 1]
                if part_:
                    sign = 1 - 2 * bit_of(bit)
                    real, imag = scaled(real, sign), scaled(imag, sign)
                base = part_ * width2
                mix[stage, pl.ds(base, width), pl.ds(0, width)] = real
                mix[stage, pl.ds(base, width), pl.ds(width, width)] = imag
                mix[stage, pl.ds(base + width, width), pl.ds(0, width)] = -imag
                mix[stage, pl.ds(base + width, width), pl.ds(width, width)] = real

    number_low, number_high, number_split = (
        stages,
        stages + 1,
        stages + 2 + len(gathers),
    )

    def build_mixz():
        sign = 1 - 2 * bit_of(low_bit)
        for part_ in range(2):
            real, imag = gates[number_low, part_, 0], gates[number_low, part_, 1]
            for column in range(2):
                line = part_ ^ column
                r, i = real, imag
                if part_:
                    flip = sign if column == 0 else -sign
                    r, i = scaled(real, flip), scaled(imag, flip)
                base, lane = line * width2, column * width2
                mixz[pl.ds(base, width), pl.ds(lane, width)] = r
                mixz[pl.ds(base, width), pl.ds(lane + width, width)] = i
                mixz[pl.ds(base + width, width), pl.ds(lane, width)] = -i
                mixz[pl.ds(base + width, width), pl.ds(lane + width, width)] = r

    def build_back():
        bits = [(split_bit, number_split, 1)] + [(bit, number, -1) for bit, number in gathers]
        bits.append((high_bit, number_high, -1))
        for step, (bit, number, way) in enumerate(bits):
            for part_ in range(2):
                real, imag = gates[number, part_, 0], gates[number, part_, 1]
                if part_:
                    sign = way * (1 - 2 * bit_of(bit))
                    real, imag = scaled(real, sign), scaled(imag, sign)
                back[step, part_, pl.ds(0, width), pl.ds(0, width)] = real
                back[step, part_, pl.ds(0, width), pl.ds(width, width)] = -imag
                back[step, part_, pl.ds(width, width), pl.ds(0, width)] = imag
                back[step, part_, pl.ds(width, width), pl.ds(width, width)] = real

    def apply(step, part_, values):
        if amps % 128 or len(values) == 1:
            return [
                jnp.dot(back[step, part_], value, preferred_element_type=jnp.float32)
                for value in values
            ]
        product = jnp.dot(
            back[step, part_],
            jnp.concatenate(values, axis=1),
            preferred_element_type=jnp.float32,
        )
        return [product[:, k * amps : (k + 1) * amps] for k in range(len(values))]

    def rounded(values):
        return [value.astype(jnp.bfloat16) for value in values]

    def both(values):
        return apply(0, 0, values), apply(0, 1, values)

    def put(slot, values):
        for s, value in enumerate(values):
            top, bottom = pl.ds(s * width2, width), pl.ds(s * width2 + width, width)
            real, imag = value[:width], value[width:]
            wb[slot, top, pl.ds(0, amps)] = real
            wb[slot, top, pl.ds(amps, amps)] = imag
            wb[slot, bottom, pl.ds(0, amps)] = -imag
            wb[slot, bottom, pl.ds(amps, amps)] = real

    def pull_one(slot, group, side, place):
        value = vb[slot]
        (same,), (swap,) = both([value])
        same = same.astype(jnp.bfloat16)
        swap = (-swap if side else swap).astype(jnp.bfloat16)
        values = [swap, same] if side else [same, swap]
        for step in reversed(range(len(gathers))):
            matrix = back[1 + step, (group >> step) & 1]
            values = rounded(
                [jnp.dot(matrix, value, preferred_element_type=jnp.float32) for value in values]
            )
        put(slot, rounded([apply(1 + len(gathers), place >> 1, [value])[0] for value in values]))

    def pull(side, place):
        if groups > 2:
            @pl.loop(0, groups)
            def _(group):
                pull_one(group * 8 + side * 4 + place, group, side, place)

            return
        values = [vb[slot_of(group, side, place)] for group in range(groups)]
        same, swap = both(values)
        same = rounded(same)
        if side:
            swap = [-value for value in swap]
        swap = rounded(swap)
        by_side = [swap, same] if side else [same, swap]
        for step in reversed(range(len(gathers))):
            fresh = [[None] * groups, [None] * groups]
            for part_ in range(2):
                keys = [(s, g) for s in range(2) for g in range(groups) if (g >> step) & 1 == part_]
                results = rounded(apply(1 + step, part_, [by_side[s][g] for s, g in keys]))
                for (s, g), value in zip(keys, results):
                    fresh[s][g] = value
            by_side = fresh
        keys = [(s, g) for s in range(2) for g in range(groups)]
        results = rounded(
            apply(1 + len(gathers), place >> 1, [by_side[s][g] for s, g in keys])
        )
        for g in range(groups):
            put(slot_of(g, side, place), [results[s * groups + g] for s in range(2)])

    def p_copy(slot):
        group, rest = divmod(slot, 8)
        flips = [bit for step, (bit, _) in enumerate(gathers) if (group >> step) & 1]
        flips += [split_bit] if rest & 4 else []
        flips += [low_bit] if rest & 1 else []
        flips += [high_bit] if rest & 2 else []
        return pltpu.make_async_remote_copy(
            src_ref=part.at[slot],
            dst_ref=red.at[slot],
            send_sem=meet_sem.at[0],
            recv_sem=meet_sem.at[1],
            device_id=far(*flips),
            device_id_type=MESH,
        )

    def body(role):
        kept = I if role == INNER else O
        counts = {}
        begun = set()

        def start_slot(hop, source, landing, piece):
            slot_copy(role, hop, source, landing, piece).start()
            key = SEND_O if piece == O else SEND_I
            if piece == V:
                key = SEND_V if hop < GATHER else SEND_SHARED
            counts[key] = counts.get(key, 0) + 1

        def share(slot, piece):
            if piece not in (V, kept):
                return
            group = slot // 8
            for step in range(group.bit_length(), len(gathers)):
                start_slot(GATHER + step, slot, slot + 8 * (1 << step), piece)

        def forward(side, place, piece):
            slot = slot_of(0, side, place)
            if piece != V or side == 0:
                if role == OUTER:
                    if place == 0:
                        start_slot(LOW, slot, slot + 1, piece)
                else:
                    if place == 0:
                        start_slot(ACROSS, slot, slot + 3, piece)
                    if place == 1:
                        start_slot(ACROSS, slot, slot + 1, piece)
                    if place != 1 and piece != I:
                        start_slot(LOW, slot, slot_of(0, side, {0: 1, 3: 2, 2: 3}[place]), piece)
            if piece == V and side == 0:
                start_slot(SPLIT, slot, slot + 4, piece)
            share(slot, piece)

        def land(slot, piece):
            slot_copy(role, ACROSS, slot, slot, piece).wait_recv()

        def got(side, place, piece):
            land(slot_of(0, side, place), piece)
            forward(side, place, piece)

        def got_shared(side, place, piece):
            for group in range(1, groups):
                slot = slot_of(group, side, place)
                land(slot, piece)
                share(slot, piece)

        def y_section(stage, side, chunk):
            y_copy(stage, side, chunk).wait_recv()
            here = pl.ds(*chunks[chunk][1:])
            joined = jnp.concatenate([xa[stage, side, here], yr[stage, side, here]], axis=-1)
            xa[stage + 1, side, here] = jnp.dot(
                joined, mix[stage], preferred_element_type=jnp.float32
            ).astype(jnp.bfloat16)
            if stage + 1 < stages:
                y_copy(stage + 1, side, chunk).start()
            elif chunks[chunk][0] != role:
                z_copy(side, chunk).start()

        def z_section(side, chunk):
            z_copy(side, chunk).wait_recv()
            here = pl.ds(*chunks[chunk][1:])
            joined = jnp.concatenate([xa[stages, side, here], zr[side, here]], axis=-1)
            for column in range(2):
                x2[column, here, pl.ds(side * width2, width2)] = jnp.dot(
                    joined,
                    mixz[:, pl.ds(column * width2, width2)],
                    preferred_element_type=jnp.float32,
                ).astype(jnp.bfloat16)

        def relay(chunk):
            x_copy(chunk).wait_recv()
            y_copy(0, 1, chunk).start()

        def weigh(slot, here, projected, fresh):
            weight = ub[slot, here].astype(jnp.float32)
            pr, pi = projected[:, :amps], projected[:, amps:]
            ur, ui = weight[:, :amps], weight[:, amps:]
            real = jnp.sum(ur * pr - ui * pi, axis=0, keepdims=True)
            imag = jnp.sum(ur * pi + ui * pr, axis=0, keepdims=True)
            if fresh:
                part[slot, 0:1] = real
                part[slot, 1:2] = imag
            else:
                part[slot, 0:1] += real
                part[slot, 1:2] += imag

        def close(items, start, size, sides):
            here = pl.ds(start, size)
            lanes = pl.ds(sides[0] * width2, len(sides) * width2)
            if groups > 2:
                for side, place, fresh in items:
                    @pl.loop(0, groups)
                    def _(group):
                        slot = group * 8 + side * 4 + place
                        projected = jnp.dot(
                            x2[place & 1, here, lanes],
                            wb[slot, lanes],
                            preferred_element_type=jnp.float32,
                        )
                        weigh(slot, here, projected, fresh)

                return
            for parity in range(2):
                members = [
                    (slot_of(group, side, place), fresh)
                    for side, place, fresh in items
                    if place & 1 == parity
                    for group in range(groups)
                ]
                for base in range(0, len(members), 4):
                    batch = members[base : base + 4]
                    projected = jnp.dot(
                        x2[parity, here, lanes],
                        jnp.concatenate([wb[slot, lanes] for slot, _ in batch], axis=1),
                        preferred_element_type=jnp.float32,
                    )
                    for k, (slot, fresh) in enumerate(batch):
                        weigh(slot, here, projected[:, 2 * amps * k : 2 * amps * (k + 1)], fresh)

        def report(side, place):
            for group in range(groups):
                slot = slot_of(group, side, place)
                if slot:
                    p_copy(slot).start()

        for kind, which in FIRST:
            if kind == U:
                span = pl.ds(0, low) if which == O else pl.ds(low, half - low)
                slot_copy(role, SPLIT, 0, 4, which, src=uo.at[span]).start()
            elif kind == Y:
                y_copy(0, 0, which).start()
            elif kind == R:
                x_copy(which).start()
            else:
                forward(0, 0, which)

        g_load.wait()
        build_mix()
        needed = [chunk for chunk in range(len(chunks)) if chunks[chunk][0] == role]
        first = chunks[needed[0]][1]
        total = sum(chunks[chunk][2] for chunk in needed)
        head = total - chunks[needed[-1]][2] if role == INNER else total
        spans = {0: (first, total, (0,)), 1: (first, head, (1,)), 2: (first + head, total - head, (1,))}
        waiting = []
        last_part = 2 if role == INNER else 1

        def flush():
            for part_ in range(3):
                items = []
                for side, place, at_part in waiting:
                    if at_part == part_:
                        items.append((side, place, (side, place) not in begun))
                        begun.add((side, place))
                if items:
                    close(items, *spans[part_])
            for side, place, part_ in waiting:
                done[side, place] = done.get((side, place), 0) + 1
                if done[side, place] == last_part + 1:
                    report(side, place)
            waiting.clear()

        done = {}
        actions = {
            Z: z_section, R: relay, G: got, S: got_shared, U: pull, F: lambda: forward(0, 0, I),
        }
        for place, (kind, *args) in enumerate(ORDERS[role]):
            if kind == C:
                waiting.append(tuple(args))
                continue
            flush()
            if kind == U and U not in begun:
                begun.add(U)
                build_back()
            if kind == Z and Z not in begun:
                begun.add(Z)
                build_mixz()
            if kind == Y:
                for stage in range(stages):
                    y_section(stage, *args)
            else:
                actions[kind](*args)
        flush()

        def drain(index, ref):
            pltpu.make_async_copy(ref, ref, send_sem.at[index]).wait()

        drain(SEND_X, xo)
        drain(SEND_U, uo)
        for stage in range(stages):
            drain(SEND_Y + stage, xa.at[stage])
        away = pl.ds(0, low) if role == INNER else pl.ds(low, half - low)
        drain(SEND_Z, zr.at[:, away])
        for index, count_ in counts.items():
            if index in (SEND_V, SEND_SHARED):
                drain(index, vb.at[pl.ds(0, count_)])
            elif index == SEND_O:
                drain(index, ub.at[pl.ds(0, count_), pl.ds(0, low)])
            else:
                drain(index, ub.at[pl.ds(0, count_), pl.ds(low, half - low)])

    @pl.when(is_inner)
    def _():
        body(INNER)

    @pl.when(jnp.logical_not(is_inner))
    def _():
        body(OUTER)

    def meet(index, ref):
        pltpu.make_async_copy(ref, ref, meet_sem.at[index]).wait()

    result = part[0]
    meet(1, red.at[pl.ds(1, slots - 1)])
    for slot in range(1, slots):
        result = result + red[slot]
    size_x, size_y = lax.axis_size("sx"), lax.axis_size("sy")
    count = size_x * size_y
    rank = coords["sx"] * size_y + coords["sy"]
    every[pl.ds(rank, 1)] = result[None]

    def flipped(axis, mask):
        where = coords[axis]
        for bit in range(mask.bit_length()):
            if (mask >> bit) & 1:
                where = where + (1 << bit) * (1 - 2 * bit_of((axis, bit)))
        return where

    def b_copy(other):
        return pltpu.make_async_remote_copy(
            src_ref=every.at[rank],
            dst_ref=every.at[rank],
            send_sem=meet_sem.at[2],
            recv_sem=meet_sem.at[3],
            device_id=other,
            device_id_type=MESH,
        )

    if count <= 32:
        across_x = [flipped("sx", mask) for mask in range(size_x)]
        across_y = [flipped("sy", mask) for mask in range(size_y)]
        for mask in reversed(range(1, count)):
            b_copy((across_x[mask // size_y], across_y[mask % size_y])).start()
    else:

        @pl.loop(1, count)
        def _(offset):
            other = (rank + offset) % count
            b_copy((other // size_y, other % size_y)).start()

    meet(0, part.at[pl.ds(1, slots - 1)])
    meet(2, every.at[pl.ds(1, count - 1)])
    meet(3, every.at[pl.ds(1, count - 1)])

    out_ref[0] = every[:, 0, :]
    out_ref[1] = every[:, 1, :]


def local(tensors, gates, closing_rows, closing_columns):
    current = tensors[:, 0, 0]
    rows, width = current.shape[1:]
    amps = closing_rows.shape[1]
    half = rows // 2
    bits_x = lax.axis_size("sx").bit_length() - 1
    bits_y = lax.axis_size("sy").bit_length() - 1
    exchanges = [(("sx", pos), pos) for pos in range(bits_x - 2)]
    gathers = [(("sy", pos), bits_x + pos) for pos in range(bits_y - 1)]
    plan = (exchanges, ("sx", bits_x - 2), ("sx", bits_x - 1), ("sy", bits_y - 1), gathers)
    stages, steps = len(exchanges), len(gathers)
    slots = 8 << steps
    count = lax.axis_size("sx") * lax.axis_size("sy")
    chunks = len(row_chunks(half))
    closed = pl.pallas_call(
        functools.partial(kernel, plan),
        out_shape=jax.ShapeDtypeStruct((2, count, amps), jnp.float32),
        in_specs=[pl.BlockSpec(memory_space=pl.ANY)] * 4,
        out_specs=pl.BlockSpec(memory_space=pltpu.VMEM),
        scratch_shapes=[
            pltpu.VMEM((stages + 1, 2, half, 2 * width), jnp.bfloat16),
            pltpu.VMEM((half, 2 * width), jnp.bfloat16),
            pltpu.VMEM((stages, 2, half, 2 * width), jnp.bfloat16),
            pltpu.VMEM((2, half, 2 * width), jnp.bfloat16),
            pltpu.VMEM((2, half, 4 * width), jnp.bfloat16),
            pltpu.VMEM((2, 2, amps, half), jnp.bfloat16),
            pltpu.VMEM((half, 2 * amps), jnp.bfloat16),
            pltpu.VMEM((slots, half, 2 * amps), jnp.bfloat16),
            pltpu.VMEM((2, amps, width), jnp.float32),
            pltpu.VMEM((slots, 2 * width, amps), jnp.bfloat16),
            pltpu.VMEM(gates.shape, jnp.bfloat16),
            pltpu.VMEM((stages, 4 * width, 2 * width), jnp.bfloat16),
            pltpu.VMEM((4 * width, 4 * width), jnp.bfloat16),
            pltpu.VMEM((2 + steps, 2, 2 * width, 2 * width), jnp.bfloat16),
            pltpu.VMEM((slots, 4 * width, 2 * amps), jnp.bfloat16),
            pltpu.VMEM((slots, 2, amps), jnp.float32),
            pltpu.VMEM((slots, 2, amps), jnp.float32),
            pltpu.VMEM((count, 2, amps), jnp.float32),
            pltpu.SemaphoreType.DMA((6,)),
            pltpu.SemaphoreType.DMA((7 + stages,)),
            pltpu.SemaphoreType.DMA((chunks,)),
            pltpu.SemaphoreType.DMA((stages, 2, chunks)),
            pltpu.SemaphoreType.DMA((2, chunks)),
            pltpu.SemaphoreType.DMA((2 * slots + 5,)),
            pltpu.SemaphoreType.DMA((4,)),
        ],
        compiler_params=pltpu.CompilerParams(
            collective_id=0, has_side_effects=True, vmem_limit_bytes=62 * 2**20
        ),
    )(current, gates, closing_rows, closing_columns)
    return closed.reshape(2, count * amps)


def solution(mesh):
    placed = (
        P(None, "sx", "sy", None, None),
        P(),
        P(None, ("sx", "sy"), None),
        P(None, ("sx", "sy"), None),
    )
    return jax.shard_map(local, mesh=mesh, in_specs=placed, out_specs=P(), check_vma=False)
```

```python
import functools

import jax
import jax.numpy as jnp
from jax import lax
from jax.experimental import pallas as pl
from jax.experimental.pallas import tpu as pltpu
from jax.sharding import PartitionSpec as P

MESH = pl.DeviceIdType.MESH
V, O, I = 0, 1, 2
INNER, OUTER = 0, 1
Y, Z, R, G, S, U, C, F = range(8)
FIRST = (
    (U, O), (U, I), (Y, 0), (Y, 1), (Y, 2), (Y, 3), (Y, 4), (R, 0), (R, 1), (F, V), (F, O),
    (R, 3), (R, 4), (R, 2),
)
ORDERS = (
    (
        (S, 0, 0, V), (U, 0, 0), (G, 1, 0, O), (G, 0, 3, V), (Y, 0, 0), (S, 0, 3, V),
        (G, 0, 1, V), (F,), (Y, 0, 1), (S, 0, 1, V), (U, 0, 1), (G, 0, 1, O), (G, 1, 0, I),
        (G, 1, 3, O), (G, 0, 3, O), (Y, 0, 2), (S, 1, 0, I), (R, 0), (Y, 0, 3), (G, 0, 2, V),
        (G, 0, 1, I), (R, 1), (Y, 0, 4), (G, 1, 1, O), (S, 0, 2, V), (U, 0, 2), (G, 0, 3, I),
        (G, 1, 0, V), (Y, 1, 0), (S, 0, 0, I), (S, 0, 1, I), (U, 0, 3), (G, 0, 2, O), (R, 3),
        (Y, 1, 1), (Z, 0, 1), (R, 4), (S, 0, 3, I), (S, 1, 0, V), (U, 1, 0), (Z, 0, 2),
        (G, 1, 3, I), (Y, 1, 3), (R, 2), (Z, 0, 0), (C, 0, 0, 0), (C, 1, 0, 0), (Y, 1, 4),
        (C, 0, 1, 0), (C, 0, 3, 0), (G, 0, 2, I), (G, 1, 3, V), (G, 1, 1, I), (S, 0, 2, I),
        (C, 0, 2, 0), (Y, 1, 2), (S, 1, 3, V), (U, 1, 3), (G, 1, 1, V), (S, 1, 1, I),
        (Z, 1, 0), (G, 1, 2, O), (S, 1, 3, I), (C, 1, 3, 0), (S, 1, 1, V), (U, 1, 1),
        (C, 1, 1, 0), (G, 1, 2, V), (Z, 1, 1), (C, 0, 0, 1), (C, 0, 1, 1), (C, 1, 1, 1),
        (C, 1, 3, 1), (C, 0, 2, 1), (C, 1, 0, 1), (G, 1, 2, I), (S, 1, 2, V), (U, 1, 2),
        (Z, 1, 2), (C, 0, 1, 2), (C, 0, 2, 2), (C, 0, 3, 2), (C, 1, 1, 2), (C, 1, 3, 2),
        (C, 1, 0, 2), (S, 1, 2, I), (C, 1, 2, 1), (C, 1, 2, 2), (C, 1, 2, 0), (C, 0, 0, 2),
        (C, 0, 3, 1),
    ),
    (
        (F,), (S, 0, 0, O), (S, 0, 0, V), (U, 0, 0), (G, 0, 1, V), (G, 1, 0, O), (Y, 0, 0),
        (S, 1, 0, O), (G, 0, 1, O), (S, 0, 1, V), (U, 0, 1), (S, 0, 1, O), (Y, 0, 1),
        (G, 1, 1, O), (Y, 0, 2), (G, 1, 0, I), (R, 0), (G, 0, 2, V), (S, 0, 2, V), (U, 0, 2),
        (G, 1, 2, O), (R, 1), (Y, 0, 4), (S, 1, 2, O), (Y, 0, 3), (G, 0, 2, O), (G, 1, 0, V),
        (Y, 1, 0), (S, 1, 0, V), (S, 0, 2, O), (U, 1, 0), (R, 3), (Y, 1, 1), (R, 4),
        (G, 0, 3, V), (Z, 0, 3), (S, 0, 3, V), (U, 0, 3), (Y, 1, 3), (R, 2), (Z, 0, 4),
        (C, 0, 0, 0), (C, 0, 1, 0), (C, 0, 2, 0), (G, 0, 3, O), (C, 1, 0, 0), (Y, 1, 4),
        (S, 0, 3, O), (C, 0, 3, 0), (G, 1, 1, V), (S, 1, 1, V), (Y, 1, 2), (U, 1, 1),
        (G, 1, 2, V), (Z, 1, 3), (Z, 1, 4), (C, 0, 1, 1), (C, 0, 3, 1), (C, 0, 0, 1),
        (S, 1, 2, V), (U, 1, 2), (G, 1, 3, V), (C, 1, 2, 1), (C, 1, 2, 0), (G, 1, 3, O),
        (S, 1, 1, O), (C, 1, 1, 1), (C, 0, 2, 1), (C, 1, 0, 1), (C, 1, 1, 0), (S, 1, 3, V),
        (U, 1, 3), (S, 1, 3, O), (C, 1, 3, 1), (C, 1, 3, 0),
    ),
)


def outer_rows(half):
    return max(16, half * 11 // 32 // 16 * 16)


def cut(start, size, pieces):
    units = size // 16
    marks = [start + 16 * (units * k // pieces) for k in range(pieces)] + [start + size]
    return [(marks[k], marks[k + 1] - marks[k]) for k in range(pieces) if marks[k + 1] > marks[k]]


def row_chunks(half):
    low = outer_rows(half)
    return [(INNER, *span) for span in cut(low, half - low, 3)] + [
        (OUTER, *span) for span in cut(0, low, 2)
    ]


def kernel(
    plan,
    x_hbm,
    g_hbm,
    u_hbm,
    v_hbm,
    out_ref,
    xa,
    xo,
    yr,
    zr,
    x2,
    uraw,
    uo,
    ub,
    vraw,
    vb,
    gates,
    mix,
    mixz,
    back,
    wb,
    part,
    red,
    every,
    local_sem,
    send_sem,
    xrecv,
    yrecv,
    zrecv,
    grecv,
    meet_sem,
):
    exchanges, low_bit, high_bit, split_bit, gathers = plan
    half, width2 = xo.shape
    width = width2 // 2
    amps = vb.shape[2]
    slots = vb.shape[0]
    groups = slots // 8
    stages = len(exchanges)
    chunks = row_chunks(half)
    low = outer_rows(half)
    coords = {"sx": lax.axis_index("sx"), "sy": lax.axis_index("sy")}

    def bit_of(bit):
        return (coords[bit[0]] // (1 << bit[1])) % 2

    def far(*flips):
        where = dict(coords)
        for bit in flips:
            where[bit[0]] = where[bit[0]] + (1 << bit[1]) * (1 - 2 * bit_of(bit))
        return (where["sx"], where["sy"])

    is_inner = bit_of(low_bit) != bit_of(high_bit)
    mine = bit_of(split_bit)
    own_rows = pl.ds(pl.multiple_of(mine * half, half), half)
    other_rows = pl.ds(pl.multiple_of((1 - mine) * half, half), half)

    def load(src, dst, index):
        copy = pltpu.make_async_copy(src, dst, local_sem.at[index])
        copy.start()
        return copy

    v_load = load(v_hbm, vraw, 0)
    u_loads = [
        load(u_hbm.at[:, :, own_rows], uraw.at[0], 1),
        load(u_hbm.at[:, :, other_rows], uraw.at[1], 2),
    ]
    for piece in range(2):
        lanes = pl.ds(piece * width, width)
        load(x_hbm.at[piece, own_rows], xa.at[0, 0, :, lanes], 3)
        load(x_hbm.at[piece, other_rows], xo.at[:, lanes], 4)
    g_load = load(g_hbm, gates, 5)

    barrier = pltpu.get_barrier_semaphore()
    peers = [bit for bit, _ in exchanges] + [low_bit, split_bit] + [bit for bit, _ in gathers]
    for bit in peers:
        pl.semaphore_signal(barrier, inc=1, device_id=far(bit), device_id_type=MESH)

    @pl.when(is_inner)
    def _():
        pl.semaphore_signal(barrier, inc=1, device_id=far(low_bit, high_bit), device_id_type=MESH)

    v_load.wait()
    for piece in range(2):
        vb[0, pl.ds(piece * width, width)] = vraw[piece].T.astype(jnp.bfloat16)
    for index in (1, 0):
        u_loads[index].wait()
        for piece in range(2):
            lanes = pl.ds(piece * amps, amps)
            if index:
                uo[:, lanes] = uraw[1, piece].T
            else:
                ub[0, :, lanes] = uraw[0, piece].T
    pltpu.make_async_copy(xa.at[0, 0], xa.at[0, 0], local_sem.at[3]).wait()
    pltpu.make_async_copy(xo, xo, local_sem.at[4]).wait()

    @pl.when(is_inner)
    def _():
        pl.semaphore_wait(barrier, len(peers) + 1)

    @pl.when(jnp.logical_not(is_inner))
    def _():
        pl.semaphore_wait(barrier, len(peers))

    def slot_of(group, side, place):
        return group * 8 + side * 4 + place

    def area(slot, piece):
        if piece == V:
            return vb.at[slot]
        if piece == O:
            return ub.at[slot, pl.ds(0, low)]
        return ub.at[slot, pl.ds(low, half - low)]

    LOW, ACROSS, SPLIT, GATHER = 0, 1, 2, 3
    SEND_X, SEND_U, SEND_Z, SEND_V, SEND_SHARED, SEND_O, SEND_I, SEND_Y = range(8)

    def landing_sem(role, slot, piece):
        if piece == V:
            return grecv.at[slot - 1]
        if piece == (I if role == INNER else O):
            return grecv.at[slots - 1 + slot - 1]
        return grecv.at[2 * (slots - 1) + slot - 1]

    def hop_device(hop):
        if hop == LOW:
            return far(low_bit)
        if hop == ACROSS:
            return far(low_bit, high_bit)
        if hop == SPLIT:
            return far(split_bit)
        return far(gathers[hop - GATHER][0])

    def slot_copy(role, hop, source, landing, piece, src=None):
        if src is not None:
            sender = SEND_U
        elif piece == V:
            sender = SEND_V if hop < GATHER else SEND_SHARED
        else:
            sender = SEND_O if piece == O else SEND_I
        return pltpu.make_async_remote_copy(
            src_ref=area(source, piece) if src is None else src,
            dst_ref=area(landing, piece),
            send_sem=send_sem.at[sender],
            recv_sem=landing_sem(1 - role if hop == LOW else role, landing, piece),
            device_id=hop_device(hop),
            device_id_type=MESH,
        )

    def x_copy(chunk):
        here = pl.ds(*chunks[chunk][1:])
        return pltpu.make_async_remote_copy(
            src_ref=xo.at[here],
            dst_ref=xa.at[0, 1, here],
            send_sem=send_sem.at[SEND_X],
            recv_sem=xrecv.at[chunk],
            device_id=far(split_bit),
            device_id_type=MESH,
        )

    def y_copy(stage, side, chunk):
        here = pl.ds(*chunks[chunk][1:])
        return pltpu.make_async_remote_copy(
            src_ref=xa.at[stage, side, here],
            dst_ref=yr.at[stage, side, here],
            send_sem=send_sem.at[SEND_Y + stage],
            recv_sem=yrecv.at[stage, side, chunk],
            device_id=far(exchanges[stage][0]),
            device_id_type=MESH,
        )

    def z_copy(side, chunk):
        here = pl.ds(*chunks[chunk][1:])
        return pltpu.make_async_remote_copy(
            src_ref=xa.at[stages, side, here],
            dst_ref=zr.at[side, here],
            send_sem=send_sem.at[SEND_Z],
            recv_sem=zrecv.at[side, chunk],
            device_id=far(low_bit),
            device_id_type=MESH,
        )

    def scaled(value, sign):
        return value * sign.astype(jnp.float32).astype(jnp.bfloat16)

    def build_mix():
        for stage, (bit, number) in enumerate(exchanges):
            for part_ in range(2):
                real, imag = gates[number, part_, 0], gates[number, part_, 1]
                if part_:
                    sign = 1 - 2 * bit_of(bit)
                    real, imag = scaled(real, sign), scaled(imag, sign)
                base = part_ * width2
                mix[stage, pl.ds(base, width), pl.ds(0, width)] = real
                mix[stage, pl.ds(base, width), pl.ds(width, width)] = imag
                mix[stage, pl.ds(base + width, width), pl.ds(0, width)] = -imag
                mix[stage, pl.ds(base + width, width), pl.ds(width, width)] = real

    number_low, number_high, number_split = (
        stages,
        stages + 1,
        stages + 2 + len(gathers),
    )

    def build_mixz():
        sign = 1 - 2 * bit_of(low_bit)
        for part_ in range(2):
            real, imag = gates[number_low, part_, 0], gates[number_low, part_, 1]
            for column in range(2):
                line = part_ ^ column
                r, i = real, imag
                if part_:
                    flip = sign if column == 0 else -sign
                    r, i = scaled(real, flip), scaled(imag, flip)
                base, lane = line * width2, column * width2
                mixz[pl.ds(base, width), pl.ds(lane, width)] = r
                mixz[pl.ds(base, width), pl.ds(lane + width, width)] = i
                mixz[pl.ds(base + width, width), pl.ds(lane, width)] = -i
                mixz[pl.ds(base + width, width), pl.ds(lane + width, width)] = r

    def build_back():
        bits = [(split_bit, number_split, 1)] + [(bit, number, -1) for bit, number in gathers]
        bits.append((high_bit, number_high, -1))
        for step, (bit, number, way) in enumerate(bits):
            for part_ in range(2):
                real, imag = gates[number, part_, 0], gates[number, part_, 1]
                if part_:
                    sign = way * (1 - 2 * bit_of(bit))
                    real, imag = scaled(real, sign), scaled(imag, sign)
                back[step, part_, pl.ds(0, width), pl.ds(0, width)] = real
                back[step, part_, pl.ds(0, width), pl.ds(width, width)] = -imag
                back[step, part_, pl.ds(width, width), pl.ds(0, width)] = imag
                back[step, part_, pl.ds(width, width), pl.ds(width, width)] = real

    def apply(step, part_, values):
        if amps % 128 or len(values) == 1:
            return [
                jnp.dot(back[step, part_], value, preferred_element_type=jnp.float32)
                for value in values
            ]
        product = jnp.dot(
            back[step, part_],
            jnp.concatenate(values, axis=1),
            preferred_element_type=jnp.float32,
        )
        return [product[:, k * amps : (k + 1) * amps] for k in range(len(values))]

    def rounded(values):
        return [value.astype(jnp.bfloat16) for value in values]

    def both(values):
        return apply(0, 0, values), apply(0, 1, values)

    def put(slot, values):
        for s, value in enumerate(values):
            top, bottom = pl.ds(s * width2, width), pl.ds(s * width2 + width, width)
            real, imag = value[:width], value[width:]
            wb[slot, top, pl.ds(0, amps)] = real
            wb[slot, top, pl.ds(amps, amps)] = imag
            wb[slot, bottom, pl.ds(0, amps)] = -imag
            wb[slot, bottom, pl.ds(amps, amps)] = real

    def pull_one(slot, group, side, place):
        value = vb[slot]
        (same,), (swap,) = both([value])
        same = same.astype(jnp.bfloat16)
        swap = (-swap if side else swap).astype(jnp.bfloat16)
        values = [swap, same] if side else [same, swap]
        for step in reversed(range(len(gathers))):
            matrix = back[1 + step, (group >> step) & 1]
            values = rounded(
                [jnp.dot(matrix, value, preferred_element_type=jnp.float32) for value in values]
            )
        put(slot, rounded([apply(1 + len(gathers), place >> 1, [value])[0] for value in values]))

    def pull(side, place):
        if groups > 2:
            @pl.loop(0, groups)
            def _(group):
                pull_one(group * 8 + side * 4 + place, group, side, place)

            return
        values = [vb[slot_of(group, side, place)] for group in range(groups)]
        same, swap = both(values)
        same = rounded(same)
        if side:
            swap = [-value for value in swap]
        swap = rounded(swap)
        by_side = [swap, same] if side else [same, swap]
        for step in reversed(range(len(gathers))):
            fresh = [[None] * groups, [None] * groups]
            for part_ in range(2):
                keys = [(s, g) for s in range(2) for g in range(groups) if (g >> step) & 1 == part_]
                results = rounded(apply(1 + step, part_, [by_side[s][g] for s, g in keys]))
                for (s, g), value in zip(keys, results):
                    fresh[s][g] = value
            by_side = fresh
        keys = [(s, g) for s in range(2) for g in range(groups)]
        results = rounded(
            apply(1 + len(gathers), place >> 1, [by_side[s][g] for s, g in keys])
        )
        for g in range(groups):
            put(slot_of(g, side, place), [results[s * groups + g] for s in range(2)])

    def p_copy(slot):
        group, rest = divmod(slot, 8)
        flips = [bit for step, (bit, _) in enumerate(gathers) if (group >> step) & 1]
        flips += [split_bit] if rest & 4 else []
        flips += [low_bit] if rest & 1 else []
        flips += [high_bit] if rest & 2 else []
        return pltpu.make_async_remote_copy(
            src_ref=part.at[slot],
            dst_ref=red.at[slot],
            send_sem=meet_sem.at[0],
            recv_sem=meet_sem.at[1],
            device_id=far(*flips),
            device_id_type=MESH,
        )

    def body(role):
        kept = I if role == INNER else O
        counts = {}
        begun = set()

        def start_slot(hop, source, landing, piece):
            slot_copy(role, hop, source, landing, piece).start()
            key = SEND_O if piece == O else SEND_I
            if piece == V:
                key = SEND_V if hop < GATHER else SEND_SHARED
            counts[key] = counts.get(key, 0) + 1

        def share(slot, piece):
            if piece not in (V, kept):
                return
            group = slot // 8
            for step in range(group.bit_length(), len(gathers)):
                start_slot(GATHER + step, slot, slot + 8 * (1 << step), piece)

        def forward(side, place, piece):
            slot = slot_of(0, side, place)
            if piece != V or side == 0:
                if role == OUTER:
                    if place == 0:
                        start_slot(LOW, slot, slot + 1, piece)
                else:
                    if place == 0:
                        start_slot(ACROSS, slot, slot + 3, piece)
                    if place == 1:
                        start_slot(ACROSS, slot, slot + 1, piece)
                    if place != 1 and piece != I:
                        start_slot(LOW, slot, slot_of(0, side, {0: 1, 3: 2, 2: 3}[place]), piece)
            if piece == V and side == 0:
                start_slot(SPLIT, slot, slot + 4, piece)
            share(slot, piece)

        def land(slot, piece):
            slot_copy(role, ACROSS, slot, slot, piece).wait_recv()

        def got(side, place, piece):
            land(slot_of(0, side, place), piece)
            forward(side, place, piece)

        def got_shared(side, place, piece):
            for group in range(1, groups):
                slot = slot_of(group, side, place)
                land(slot, piece)
                share(slot, piece)

        def y_section(stage, side, chunk):
            y_copy(stage, side, chunk).wait_recv()
            here = pl.ds(*chunks[chunk][1:])
            joined = jnp.concatenate([xa[stage, side, here], yr[stage, side, here]], axis=-1)
            xa[stage + 1, side, here] = jnp.dot(
                joined, mix[stage], preferred_element_type=jnp.float32
            ).astype(jnp.bfloat16)
            if stage + 1 < stages:
                y_copy(stage + 1, side, chunk).start()
            elif chunks[chunk][0] != role:
                z_copy(side, chunk).start()

        def z_section(side, chunk):
            z_copy(side, chunk).wait_recv()
            here = pl.ds(*chunks[chunk][1:])
            joined = jnp.concatenate([xa[stages, side, here], zr[side, here]], axis=-1)
            for column in range(2):
                x2[column, here, pl.ds(side * width2, width2)] = jnp.dot(
                    joined,
                    mixz[:, pl.ds(column * width2, width2)],
                    preferred_element_type=jnp.float32,
                ).astype(jnp.bfloat16)

        def relay(chunk):
            x_copy(chunk).wait_recv()
            y_copy(0, 1, chunk).start()

        def weigh(slot, here, projected, fresh):
            weight = ub[slot, here].astype(jnp.float32)
            pr, pi = projected[:, :amps], projected[:, amps:]
            ur, ui = weight[:, :amps], weight[:, amps:]
            real = jnp.sum(ur * pr - ui * pi, axis=0, keepdims=True)
            imag = jnp.sum(ur * pi + ui * pr, axis=0, keepdims=True)
            if fresh:
                part[slot, 0:1] = real
                part[slot, 1:2] = imag
            else:
                part[slot, 0:1] += real
                part[slot, 1:2] += imag

        def close(items, start, size, sides):
            here = pl.ds(start, size)
            lanes = pl.ds(sides[0] * width2, len(sides) * width2)
            if groups > 2:
                for side, place, fresh in items:
                    @pl.loop(0, groups)
                    def _(group):
                        slot = group * 8 + side * 4 + place
                        projected = jnp.dot(
                            x2[place & 1, here, lanes],
                            wb[slot, lanes],
                            preferred_element_type=jnp.float32,
                        )
                        weigh(slot, here, projected, fresh)

                return
            for parity in range(2):
                members = [
                    (slot_of(group, side, place), fresh)
                    for side, place, fresh in items
                    if place & 1 == parity
                    for group in range(groups)
                ]
                for base in range(0, len(members), 4):
                    batch = members[base : base + 4]
                    projected = jnp.dot(
                        x2[parity, here, lanes],
                        jnp.concatenate([wb[slot, lanes] for slot, _ in batch], axis=1),
                        preferred_element_type=jnp.float32,
                    )
                    for k, (slot, fresh) in enumerate(batch):
                        weigh(slot, here, projected[:, 2 * amps * k : 2 * amps * (k + 1)], fresh)

        def report(side, place):
            for group in range(groups):
                slot = slot_of(group, side, place)
                if slot:
                    p_copy(slot).start()

        for kind, which in FIRST:
            if kind == U:
                span = pl.ds(0, low) if which == O else pl.ds(low, half - low)
                slot_copy(role, SPLIT, 0, 4, which, src=uo.at[span]).start()
            elif kind == Y:
                y_copy(0, 0, which).start()
            elif kind == R:
                x_copy(which).start()
            else:
                forward(0, 0, which)

        g_load.wait()
        build_mix()
        needed = [chunk for chunk in range(len(chunks)) if chunks[chunk][0] == role]
        first = chunks[needed[0]][1]
        total = sum(chunks[chunk][2] for chunk in needed)
        head = total - chunks[needed[-1]][2] if role == INNER else total
        spans = {0: (first, total, (0,)), 1: (first, head, (1,)), 2: (first + head, total - head, (1,))}
        waiting = []
        last_part = 2 if role == INNER else 1

        def flush():
            for part_ in range(3):
                items = []
                for side, place, at_part in waiting:
                    if at_part == part_:
                        items.append((side, place, (side, place) not in begun))
                        begun.add((side, place))
                if items:
                    close(items, *spans[part_])
            for side, place, part_ in waiting:
                done[side, place] = done.get((side, place), 0) + 1
                if done[side, place] == last_part + 1:
                    report(side, place)
            waiting.clear()

        done = {}
        actions = {
            Z: z_section, R: relay, G: got, S: got_shared, U: pull, F: lambda: forward(0, 0, I),
        }
        for place, (kind, *args) in enumerate(ORDERS[role]):
            if kind == C:
                waiting.append(tuple(args))
                continue
            flush()
            if kind == U and U not in begun:
                begun.add(U)
                build_back()
            if kind == Z and Z not in begun:
                begun.add(Z)
                build_mixz()
            if kind == Y:
                for stage in range(stages):
                    y_section(stage, *args)
            else:
                actions[kind](*args)
        flush()

        def drain(index, ref):
            pltpu.make_async_copy(ref, ref, send_sem.at[index]).wait()

        drain(SEND_X, xo)
        drain(SEND_U, uo)
        for stage in range(stages):
            drain(SEND_Y + stage, xa.at[stage])
        away = pl.ds(0, low) if role == INNER else pl.ds(low, half - low)
        drain(SEND_Z, zr.at[:, away])
        for index, count_ in counts.items():
            if index in (SEND_V, SEND_SHARED):
                drain(index, vb.at[pl.ds(0, count_)])
            elif index == SEND_O:
                drain(index, ub.at[pl.ds(0, count_), pl.ds(0, low)])
            else:
                drain(index, ub.at[pl.ds(0, count_), pl.ds(low, half - low)])

    @pl.when(is_inner)
    def _():
        body(INNER)

    @pl.when(jnp.logical_not(is_inner))
    def _():
        body(OUTER)

    def meet(index, ref):
        pltpu.make_async_copy(ref, ref, meet_sem.at[index]).wait()

    result = part[0]
    meet(1, red.at[pl.ds(1, slots - 1)])
    for slot in range(1, slots):
        result = result + red[slot]
    size_x, size_y = lax.axis_size("sx"), lax.axis_size("sy")
    count = size_x * size_y
    rank = coords["sx"] * size_y + coords["sy"]
    every[pl.ds(rank, 1)] = result[None]

    def flipped(axis, mask):
        where = coords[axis]
        for bit in range(mask.bit_length()):
            if (mask >> bit) & 1:
                where = where + (1 << bit) * (1 - 2 * bit_of((axis, bit)))
        return where

    def b_copy(other):
        return pltpu.make_async_remote_copy(
            src_ref=every.at[rank],
            dst_ref=every.at[rank],
            send_sem=meet_sem.at[2],
            recv_sem=meet_sem.at[3],
            device_id=other,
            device_id_type=MESH,
        )

    if count <= 32:
        across_x = [flipped("sx", mask) for mask in range(size_x)]
        across_y = [flipped("sy", mask) for mask in range(size_y)]
        for mask in reversed(range(1, count)):
            b_copy((across_x[mask // size_y], across_y[mask % size_y])).start()
    else:

        @pl.loop(1, count)
        def _(offset):
            other = (rank + offset) % count
            b_copy((other // size_y, other % size_y)).start()

    meet(0, part.at[pl.ds(1, slots - 1)])
    meet(2, every.at[pl.ds(1, count - 1)])
    meet(3, every.at[pl.ds(1, count - 1)])

    out_ref[0] = every[:, 0, :]
    out_ref[1] = every[:, 1, :]


def local(tensors, gates, closing_rows, closing_columns):
    current = tensors[:, 0, 0]
    rows, width = current.shape[1:]
    amps = closing_rows.shape[1]
    half = rows // 2
    bits_x = lax.axis_size("sx").bit_length() - 1
    bits_y = lax.axis_size("sy").bit_length() - 1
    exchanges = [(("sx", pos), pos) for pos in range(bits_x - 2)]
    gathers = [(("sy", pos), bits_x + pos) for pos in range(bits_y - 1)]
    plan = (exchanges, ("sx", bits_x - 2), ("sx", bits_x - 1), ("sy", bits_y - 1), gathers)
    stages, steps = len(exchanges), len(gathers)
    slots = 8 << steps
    count = lax.axis_size("sx") * lax.axis_size("sy")
    chunks = len(row_chunks(half))
    grant = 55100 * 2**10 if amps % 128 == 0 else 62 * 2**20
    closed = pl.pallas_call(
        functools.partial(kernel, plan),
        out_shape=jax.ShapeDtypeStruct((2, count, amps), jnp.float32),
        in_specs=[pl.BlockSpec(memory_space=pl.ANY)] * 4,
        out_specs=pl.BlockSpec(memory_space=pltpu.VMEM),
        scratch_shapes=[
            pltpu.VMEM((stages + 1, 2, half, 2 * width), jnp.bfloat16),
            pltpu.VMEM((half, 2 * width), jnp.bfloat16),
            pltpu.VMEM((stages, 2, half, 2 * width), jnp.bfloat16),
            pltpu.VMEM((2, half, 2 * width), jnp.bfloat16),
            pltpu.VMEM((2, half, 4 * width), jnp.bfloat16),
            pltpu.VMEM((2, 2, amps, half), jnp.bfloat16),
            pltpu.VMEM((half, 2 * amps), jnp.bfloat16),
            pltpu.VMEM((slots, half, 2 * amps), jnp.bfloat16),
            pltpu.VMEM((2, amps, width), jnp.float32),
            pltpu.VMEM((slots, 2 * width, amps), jnp.bfloat16),
            pltpu.VMEM(gates.shape, jnp.bfloat16),
            pltpu.VMEM((stages, 4 * width, 2 * width), jnp.bfloat16),
            pltpu.VMEM((4 * width, 4 * width), jnp.bfloat16),
            pltpu.VMEM((2 + steps, 2, 2 * width, 2 * width), jnp.bfloat16),
            pltpu.VMEM((slots, 4 * width, 2 * amps), jnp.bfloat16),
            pltpu.VMEM((slots, 2, amps), jnp.float32),
            pltpu.VMEM((slots, 2, amps), jnp.float32),
            pltpu.VMEM((count, 2, amps), jnp.float32),
            pltpu.SemaphoreType.DMA((6,)),
            pltpu.SemaphoreType.DMA((7 + stages,)),
            pltpu.SemaphoreType.DMA((chunks,)),
            pltpu.SemaphoreType.DMA((stages, 2, chunks)),
            pltpu.SemaphoreType.DMA((2, chunks)),
            pltpu.SemaphoreType.DMA((2 * slots + 5,)),
            pltpu.SemaphoreType.DMA((4,)),
        ],
        compiler_params=pltpu.CompilerParams(
            collective_id=0, has_side_effects=True, vmem_limit_bytes=grant
        ),
    )(current, gates, closing_rows, closing_columns)
    return closed.reshape(2, count * amps)


def solution(mesh):
    placed = (
        P(None, "sx", "sy", None, None),
        P(),
        P(None, ("sx", "sy"), None),
        P(None, ("sx", "sy"), None),
    )
    return jax.shard_map(local, mesh=mesh, in_specs=placed, out_specs=P(), check_vma=False)
```

```python
import functools

import jax
import jax.numpy as jnp
from jax import lax
from jax.experimental import pallas as pl
from jax.experimental.pallas import tpu as pltpu
from jax.sharding import PartitionSpec as P

MESH = pl.DeviceIdType.MESH
V, O, I = 0, 1, 2
INNER, OUTER = 0, 1
Y, Z, R, G, S, U, C, F = range(8)
FIRST = (
    (U, O), (U, I), (Y, 0), (Y, 1), (Y, 2), (Y, 3), (Y, 4), (R, 0), (R, 1), (F, V), (F, O),
    (R, 3), (R, 4), (R, 2),
)
ORDERS = (
    (
        (S, 0, 0, V), (U, 0, 0), (G, 1, 0, O), (G, 0, 3, V), (Y, 0, 0), (S, 0, 3, V),
        (G, 0, 1, V), (F,), (Y, 0, 1), (S, 0, 1, V), (U, 0, 1), (G, 0, 1, O), (G, 1, 0, I),
        (G, 1, 3, O), (G, 0, 3, O), (Y, 0, 2), (S, 1, 0, I), (R, 0), (Y, 0, 3), (G, 0, 2, V),
        (G, 0, 1, I), (R, 1), (Y, 0, 4), (G, 1, 1, O), (S, 0, 2, V), (U, 0, 2), (G, 0, 3, I),
        (G, 1, 0, V), (Y, 1, 0), (S, 0, 0, I), (S, 0, 1, I), (U, 0, 3), (G, 0, 2, O), (R, 3),
        (Y, 1, 1), (Z, 0, 1), (R, 4), (S, 0, 3, I), (S, 1, 0, V), (U, 1, 0), (Z, 0, 2),
        (G, 1, 3, I), (Y, 1, 3), (R, 2), (Z, 0, 0), (C, 0, 0, 0), (C, 1, 0, 0), (Y, 1, 4),
        (C, 0, 1, 0), (C, 0, 3, 0), (G, 0, 2, I), (G, 1, 3, V), (G, 1, 1, I), (S, 0, 2, I),
        (C, 0, 2, 0), (Y, 1, 2), (S, 1, 3, V), (U, 1, 3), (G, 1, 1, V), (S, 1, 1, I),
        (Z, 1, 0), (G, 1, 2, O), (S, 1, 3, I), (C, 1, 3, 0), (S, 1, 1, V), (U, 1, 1),
        (C, 1, 1, 0), (G, 1, 2, V), (Z, 1, 1), (C, 0, 0, 1), (C, 0, 1, 1), (C, 1, 1, 1),
        (C, 1, 3, 1), (C, 0, 2, 1), (C, 1, 0, 1), (G, 1, 2, I), (S, 1, 2, V), (U, 1, 2),
        (Z, 1, 2), (C, 0, 1, 2), (C, 0, 2, 2), (C, 0, 3, 2), (C, 1, 1, 2), (C, 1, 3, 2),
        (C, 1, 0, 2), (S, 1, 2, I), (C, 1, 2, 1), (C, 1, 2, 2), (C, 1, 2, 0), (C, 0, 0, 2),
        (C, 0, 3, 1),
    ),
    (
        (F,), (S, 0, 0, O), (S, 0, 0, V), (U, 0, 0), (G, 0, 1, V), (G, 1, 0, O), (Y, 0, 0),
        (S, 1, 0, O), (G, 0, 1, O), (S, 0, 1, V), (U, 0, 1), (S, 0, 1, O), (Y, 0, 1),
        (G, 1, 1, O), (Y, 0, 2), (G, 1, 0, I), (R, 0), (G, 0, 2, V), (S, 0, 2, V), (U, 0, 2),
        (G, 1, 2, O), (R, 1), (Y, 0, 4), (S, 1, 2, O), (Y, 0, 3), (G, 0, 2, O), (G, 1, 0, V),
        (Y, 1, 0), (S, 1, 0, V), (S, 0, 2, O), (U, 1, 0), (R, 3), (Y, 1, 1), (R, 4),
        (G, 0, 3, V), (Z, 0, 3), (S, 0, 3, V), (U, 0, 3), (Y, 1, 3), (R, 2), (Z, 0, 4),
        (C, 0, 0, 0), (C, 0, 1, 0), (C, 0, 2, 0), (G, 0, 3, O), (C, 1, 0, 0), (Y, 1, 4),
        (S, 0, 3, O), (C, 0, 3, 0), (G, 1, 1, V), (S, 1, 1, V), (Y, 1, 2), (U, 1, 1),
        (G, 1, 2, V), (Z, 1, 3), (Z, 1, 4), (C, 0, 1, 1), (C, 0, 3, 1), (C, 0, 0, 1),
        (S, 1, 2, V), (U, 1, 2), (G, 1, 3, V), (C, 1, 2, 1), (C, 1, 2, 0), (G, 1, 3, O),
        (S, 1, 1, O), (C, 1, 1, 1), (C, 0, 2, 1), (C, 1, 0, 1), (C, 1, 1, 0), (S, 1, 3, V),
        (U, 1, 3), (S, 1, 3, O), (C, 1, 3, 1), (C, 1, 3, 0),
    ),
)


def outer_rows(half):
    return max(16, half * 11 // 32 // 16 * 16)


def cut(start, size, pieces):
    units = size // 16
    marks = [start + 16 * (units * k // pieces) for k in range(pieces)] + [start + size]
    return [(marks[k], marks[k + 1] - marks[k]) for k in range(pieces) if marks[k + 1] > marks[k]]


def row_chunks(half):
    low = outer_rows(half)
    return [(INNER, *span) for span in cut(low, half - low, 3)] + [
        (OUTER, *span) for span in cut(0, low, 2)
    ]


def kernel(
    plan,
    x_hbm,
    g_hbm,
    u_hbm,
    v_hbm,
    out_ref,
    xa,
    xo,
    yr,
    zr,
    x2,
    uraw,
    uo,
    ub,
    vraw,
    vb,
    gates,
    mix,
    mixz,
    back,
    wb,
    part,
    red,
    every,
    local_sem,
    send_sem,
    xrecv,
    yrecv,
    zrecv,
    grecv,
    meet_sem,
):
    exchanges, low_bit, high_bit, split_bit, gathers = plan
    half, width2 = xo.shape
    width = width2 // 2
    amps = vb.shape[2]
    slots = vb.shape[0]
    groups = slots // 8
    stages = len(exchanges)
    chunks = row_chunks(half)
    low = outer_rows(half)
    coords = {"sx": lax.axis_index("sx"), "sy": lax.axis_index("sy")}

    def bit_of(bit):
        return (coords[bit[0]] // (1 << bit[1])) % 2

    def far(*flips):
        where = dict(coords)
        for bit in flips:
            where[bit[0]] = where[bit[0]] + (1 << bit[1]) * (1 - 2 * bit_of(bit))
        return (where["sx"], where["sy"])

    is_inner = bit_of(low_bit) != bit_of(high_bit)
    mine = bit_of(split_bit)
    own_rows = pl.ds(pl.multiple_of(mine * half, half), half)
    other_rows = pl.ds(pl.multiple_of((1 - mine) * half, half), half)

    def load(src, dst, index):
        copy = pltpu.make_async_copy(src, dst, local_sem.at[index])
        copy.start()
        return copy

    v_load = load(v_hbm, vraw, 0)
    u_loads = [
        load(u_hbm.at[:, :, own_rows], uraw.at[0], 1),
        load(u_hbm.at[:, :, other_rows], uraw.at[1], 2),
    ]
    for piece in range(2):
        lanes = pl.ds(piece * width, width)
        load(x_hbm.at[piece, own_rows], xa.at[0, 0, :, lanes], 3)
        load(x_hbm.at[piece, other_rows], xo.at[:, lanes], 4)
    g_load = load(g_hbm, gates, 5)

    barrier = pltpu.get_barrier_semaphore()
    peers = [bit for bit, _ in exchanges] + [low_bit, split_bit] + [bit for bit, _ in gathers]
    for bit in peers:
        pl.semaphore_signal(barrier, inc=1, device_id=far(bit), device_id_type=MESH)

    @pl.when(is_inner)
    def _():
        pl.semaphore_signal(barrier, inc=1, device_id=far(low_bit, high_bit), device_id_type=MESH)

    v_load.wait()
    for piece in range(2):
        vb[0, pl.ds(piece * width, width)] = vraw[piece].T.astype(jnp.bfloat16)
    for index in (1, 0):
        u_loads[index].wait()
        for piece in range(2):
            lanes = pl.ds(piece * amps, amps)
            if index:
                uo[:, lanes] = uraw[1, piece].T
            else:
                ub[0, :, lanes] = uraw[0, piece].T
    pltpu.make_async_copy(xa.at[0, 0], xa.at[0, 0], local_sem.at[3]).wait()
    pltpu.make_async_copy(xo, xo, local_sem.at[4]).wait()

    @pl.when(is_inner)
    def _():
        pl.semaphore_wait(barrier, len(peers) + 1)

    @pl.when(jnp.logical_not(is_inner))
    def _():
        pl.semaphore_wait(barrier, len(peers))

    def slot_of(group, side, place):
        return group * 8 + side * 4 + place

    def area(slot, piece):
        if piece == V:
            return vb.at[slot]
        if piece == O:
            return ub.at[slot, pl.ds(0, low)]
        return ub.at[slot, pl.ds(low, half - low)]

    LOW, ACROSS, SPLIT, GATHER = 0, 1, 2, 3
    SEND_X, SEND_U, SEND_Z, SEND_V, SEND_SHARED, SEND_O, SEND_I, SEND_Y = range(8)

    def landing_sem(role, slot, piece):
        if piece == V:
            return grecv.at[slot - 1]
        if piece == (I if role == INNER else O):
            return grecv.at[slots - 1 + slot - 1]
        return grecv.at[2 * (slots - 1) + slot - 1]

    def hop_device(hop):
        if hop == LOW:
            return far(low_bit)
        if hop == ACROSS:
            return far(low_bit, high_bit)
        if hop == SPLIT:
            return far(split_bit)
        return far(gathers[hop - GATHER][0])

    def slot_copy(role, hop, source, landing, piece, src=None):
        if src is not None:
            sender = SEND_U
        elif piece == V:
            sender = SEND_V if hop < GATHER else SEND_SHARED
        else:
            sender = SEND_O if piece == O else SEND_I
        return pltpu.make_async_remote_copy(
            src_ref=area(source, piece) if src is None else src,
            dst_ref=area(landing, piece),
            send_sem=send_sem.at[sender],
            recv_sem=landing_sem(1 - role if hop == LOW else role, landing, piece),
            device_id=hop_device(hop),
            device_id_type=MESH,
        )

    def x_copy(chunk):
        here = pl.ds(*chunks[chunk][1:])
        return pltpu.make_async_remote_copy(
            src_ref=xo.at[here],
            dst_ref=xa.at[0, 1, here],
            send_sem=send_sem.at[SEND_X],
            recv_sem=xrecv.at[chunk],
            device_id=far(split_bit),
            device_id_type=MESH,
        )

    def y_copy(stage, side, chunk):
        here = pl.ds(*chunks[chunk][1:])
        return pltpu.make_async_remote_copy(
            src_ref=xa.at[stage, side, here],
            dst_ref=yr.at[stage, side, here],
            send_sem=send_sem.at[SEND_Y + stage],
            recv_sem=yrecv.at[stage, side, chunk],
            device_id=far(exchanges[stage][0]),
            device_id_type=MESH,
        )

    def z_copy(side, chunk):
        here = pl.ds(*chunks[chunk][1:])
        return pltpu.make_async_remote_copy(
            src_ref=xa.at[stages, side, here],
            dst_ref=zr.at[side, here],
            send_sem=send_sem.at[SEND_Z],
            recv_sem=zrecv.at[side, chunk],
            device_id=far(low_bit),
            device_id_type=MESH,
        )

    def scaled(value, sign):
        return value * sign.astype(jnp.float32).astype(jnp.bfloat16)

    def build_mix():
        for stage, (bit, number) in enumerate(exchanges):
            for part_ in range(2):
                real, imag = gates[number, part_, 0], gates[number, part_, 1]
                if part_:
                    sign = 1 - 2 * bit_of(bit)
                    real, imag = scaled(real, sign), scaled(imag, sign)
                base = part_ * width2
                mix[stage, pl.ds(base, width), pl.ds(0, width)] = real
                mix[stage, pl.ds(base, width), pl.ds(width, width)] = imag
                mix[stage, pl.ds(base + width, width), pl.ds(0, width)] = -imag
                mix[stage, pl.ds(base + width, width), pl.ds(width, width)] = real

    number_low, number_high, number_split = (
        stages,
        stages + 1,
        stages + 2 + len(gathers),
    )

    def build_mixz():
        sign = 1 - 2 * bit_of(low_bit)
        for part_ in range(2):
            real, imag = gates[number_low, part_, 0], gates[number_low, part_, 1]
            for column in range(2):
                line = part_ ^ column
                r, i = real, imag
                if part_:
                    flip = sign if column == 0 else -sign
                    r, i = scaled(real, flip), scaled(imag, flip)
                base, lane = line * width2, column * width2
                mixz[pl.ds(base, width), pl.ds(lane, width)] = r
                mixz[pl.ds(base, width), pl.ds(lane + width, width)] = i
                mixz[pl.ds(base + width, width), pl.ds(lane, width)] = -i
                mixz[pl.ds(base + width, width), pl.ds(lane + width, width)] = r

    def build_back():
        bits = [(split_bit, number_split, 1)] + [(bit, number, -1) for bit, number in gathers]
        bits.append((high_bit, number_high, -1))
        for step, (bit, number, way) in enumerate(bits):
            for part_ in range(2):
                real, imag = gates[number, part_, 0], gates[number, part_, 1]
                if part_:
                    sign = way * (1 - 2 * bit_of(bit))
                    real, imag = scaled(real, sign), scaled(imag, sign)
                back[step, part_, pl.ds(0, width), pl.ds(0, width)] = real
                back[step, part_, pl.ds(0, width), pl.ds(width, width)] = -imag
                back[step, part_, pl.ds(width, width), pl.ds(0, width)] = imag
                back[step, part_, pl.ds(width, width), pl.ds(width, width)] = real

    def apply(step, part_, values):
        if amps % 128 or len(values) == 1:
            return [
                jnp.dot(back[step, part_], value, preferred_element_type=jnp.float32)
                for value in values
            ]
        product = jnp.dot(
            back[step, part_],
            jnp.concatenate(values, axis=1),
            preferred_element_type=jnp.float32,
        )
        return [product[:, k * amps : (k + 1) * amps] for k in range(len(values))]

    def rounded(values):
        return [value.astype(jnp.bfloat16) for value in values]

    def both(values):
        return apply(0, 0, values), apply(0, 1, values)

    def put(slot, values):
        for s, value in enumerate(values):
            top, bottom = pl.ds(s * width2, width), pl.ds(s * width2 + width, width)
            real, imag = value[:width], value[width:]
            wb[slot, top, pl.ds(0, amps)] = real
            wb[slot, top, pl.ds(amps, amps)] = imag
            wb[slot, bottom, pl.ds(0, amps)] = -imag
            wb[slot, bottom, pl.ds(amps, amps)] = real

    def pull_one(slot, group, side, place):
        value = vb[slot]
        (same,), (swap,) = both([value])
        same = same.astype(jnp.bfloat16)
        swap = (-swap if side else swap).astype(jnp.bfloat16)
        values = [swap, same] if side else [same, swap]
        for step in reversed(range(len(gathers))):
            matrix = back[1 + step, (group >> step) & 1]
            values = rounded(
                [jnp.dot(matrix, value, preferred_element_type=jnp.float32) for value in values]
            )
        put(slot, rounded([apply(1 + len(gathers), place >> 1, [value])[0] for value in values]))

    def pull(side, place):
        if groups > 2:
            @pl.loop(0, groups)
            def _(group):
                pull_one(group * 8 + side * 4 + place, group, side, place)

            return
        values = [vb[slot_of(group, side, place)] for group in range(groups)]
        same, swap = both(values)
        same = rounded(same)
        if side:
            swap = [-value for value in swap]
        swap = rounded(swap)
        by_side = [swap, same] if side else [same, swap]
        for step in reversed(range(len(gathers))):
            fresh = [[None] * groups, [None] * groups]
            for part_ in range(2):
                keys = [(s, g) for s in range(2) for g in range(groups) if (g >> step) & 1 == part_]
                results = rounded(apply(1 + step, part_, [by_side[s][g] for s, g in keys]))
                for (s, g), value in zip(keys, results):
                    fresh[s][g] = value
            by_side = fresh
        keys = [(s, g) for s in range(2) for g in range(groups)]
        results = rounded(
            apply(1 + len(gathers), place >> 1, [by_side[s][g] for s, g in keys])
        )
        for g in range(groups):
            put(slot_of(g, side, place), [results[s * groups + g] for s in range(2)])

    def p_copy(slot):
        group, rest = divmod(slot, 8)
        flips = [bit for step, (bit, _) in enumerate(gathers) if (group >> step) & 1]
        flips += [split_bit] if rest & 4 else []
        flips += [low_bit] if rest & 1 else []
        flips += [high_bit] if rest & 2 else []
        return pltpu.make_async_remote_copy(
            src_ref=part.at[slot],
            dst_ref=red.at[slot],
            send_sem=meet_sem.at[0],
            recv_sem=meet_sem.at[1],
            device_id=far(*flips),
            device_id_type=MESH,
        )

    def body(role):
        kept = I if role == INNER else O
        counts = {}
        begun = set()

        def start_slot(hop, source, landing, piece):
            slot_copy(role, hop, source, landing, piece).start()
            key = SEND_O if piece == O else SEND_I
            if piece == V:
                key = SEND_V if hop < GATHER else SEND_SHARED
            counts[key] = counts.get(key, 0) + 1

        def share(slot, piece):
            if piece not in (V, kept):
                return
            group = slot // 8
            for step in range(group.bit_length(), len(gathers)):
                start_slot(GATHER + step, slot, slot + 8 * (1 << step), piece)

        def forward(side, place, piece):
            slot = slot_of(0, side, place)
            if piece != V or side == 0:
                if role == OUTER:
                    if place == 0:
                        start_slot(LOW, slot, slot + 1, piece)
                else:
                    if place == 0:
                        start_slot(ACROSS, slot, slot + 3, piece)
                    if place == 1:
                        start_slot(ACROSS, slot, slot + 1, piece)
                    if place != 1 and piece != I:
                        start_slot(LOW, slot, slot_of(0, side, {0: 1, 3: 2, 2: 3}[place]), piece)
            if piece == V and side == 0:
                start_slot(SPLIT, slot, slot + 4, piece)
            share(slot, piece)

        def land(slot, piece):
            slot_copy(role, ACROSS, slot, slot, piece).wait_recv()

        def got(side, place, piece):
            land(slot_of(0, side, place), piece)
            forward(side, place, piece)

        def got_shared(side, place, piece):
            for group in range(1, groups):
                slot = slot_of(group, side, place)
                land(slot, piece)
                share(slot, piece)

        def y_section(stage, side, chunk):
            y_copy(stage, side, chunk).wait_recv()
            here = pl.ds(*chunks[chunk][1:])
            joined = jnp.concatenate([xa[stage, side, here], yr[stage, side, here]], axis=-1)
            xa[stage + 1, side, here] = jnp.dot(
                joined, mix[stage], preferred_element_type=jnp.float32
            ).astype(jnp.bfloat16)
            if stage + 1 < stages:
                y_copy(stage + 1, side, chunk).start()
            elif chunks[chunk][0] != role:
                z_copy(side, chunk).start()

        def z_section(side, chunk):
            z_copy(side, chunk).wait_recv()
            here = pl.ds(*chunks[chunk][1:])
            joined = jnp.concatenate([xa[stages, side, here], zr[side, here]], axis=-1)
            for column in range(2):
                x2[column, here, pl.ds(side * width2, width2)] = jnp.dot(
                    joined,
                    mixz[:, pl.ds(column * width2, width2)],
                    preferred_element_type=jnp.float32,
                ).astype(jnp.bfloat16)

        def relay(chunk):
            x_copy(chunk).wait_recv()
            y_copy(0, 1, chunk).start()

        def weigh(slot, here, projected, fresh):
            weight = ub[slot, here].astype(jnp.float32)
            pr, pi = projected[:, :amps], projected[:, amps:]
            ur, ui = weight[:, :amps], weight[:, amps:]
            real = jnp.sum(ur * pr - ui * pi, axis=0, keepdims=True)
            imag = jnp.sum(ur * pi + ui * pr, axis=0, keepdims=True)
            if fresh:
                part[slot, 0:1] = real
                part[slot, 1:2] = imag
            else:
                part[slot, 0:1] += real
                part[slot, 1:2] += imag

        def close(items, start, size, sides):
            here = pl.ds(start, size)
            lanes = pl.ds(sides[0] * width2, len(sides) * width2)
            if groups > 2:
                for side, place, fresh in items:
                    @pl.loop(0, groups)
                    def _(group):
                        slot = group * 8 + side * 4 + place
                        projected = jnp.dot(
                            x2[place & 1, here, lanes],
                            wb[slot, lanes],
                            preferred_element_type=jnp.float32,
                        )
                        weigh(slot, here, projected, fresh)

                return
            for parity in range(2):
                members = [
                    (slot_of(group, side, place), fresh)
                    for side, place, fresh in items
                    if place & 1 == parity
                    for group in range(groups)
                ]
                for base in range(0, len(members), 4):
                    batch = members[base : base + 4]
                    projected = jnp.dot(
                        x2[parity, here, lanes],
                        jnp.concatenate([wb[slot, lanes] for slot, _ in batch], axis=1),
                        preferred_element_type=jnp.float32,
                    )
                    for k, (slot, fresh) in enumerate(batch):
                        weigh(slot, here, projected[:, 2 * amps * k : 2 * amps * (k + 1)], fresh)

        def report(side, place):
            for group in range(groups):
                slot = slot_of(group, side, place)
                if slot:
                    p_copy(slot).start()

        for kind, which in FIRST:
            if kind == U:
                span = pl.ds(0, low) if which == O else pl.ds(low, half - low)
                slot_copy(role, SPLIT, 0, 4, which, src=uo.at[span]).start()
            elif kind == Y:
                y_copy(0, 0, which).start()
            elif kind == R:
                x_copy(which).start()
            else:
                forward(0, 0, which)

        g_load.wait()
        build_mix()
        needed = [chunk for chunk in range(len(chunks)) if chunks[chunk][0] == role]
        first = chunks[needed[0]][1]
        total = sum(chunks[chunk][2] for chunk in needed)
        head = total - chunks[needed[-1]][2] if role == INNER else total
        spans = {0: (first, total, (0,)), 1: (first, head, (1,)), 2: (first + head, total - head, (1,))}
        waiting = []
        last_part = 2 if role == INNER else 1

        def flush():
            for part_ in range(3):
                items = []
                for side, place, at_part in waiting:
                    if at_part == part_:
                        items.append((side, place, (side, place) not in begun))
                        begun.add((side, place))
                if items:
                    close(items, *spans[part_])
            for side, place, part_ in waiting:
                done[side, place] = done.get((side, place), 0) + 1
                if done[side, place] == last_part + 1:
                    report(side, place)
            waiting.clear()

        done = {}
        actions = {
            Z: z_section, R: relay, G: got, S: got_shared, U: pull, F: lambda: forward(0, 0, I),
        }
        for place, (kind, *args) in enumerate(ORDERS[role]):
            if kind == C:
                waiting.append(tuple(args))
                continue
            flush()
            if kind == U and U not in begun:
                begun.add(U)
                build_back()
            if kind == Z and Z not in begun:
                begun.add(Z)
                build_mixz()
            if kind == Y:
                for stage in range(stages):
                    y_section(stage, *args)
            else:
                actions[kind](*args)
        flush()

        def drain(index, ref):
            pltpu.make_async_copy(ref, ref, send_sem.at[index]).wait()

        drain(SEND_X, xo)
        drain(SEND_U, uo)
        for stage in range(stages):
            drain(SEND_Y + stage, xa.at[stage])
        away = pl.ds(0, low) if role == INNER else pl.ds(low, half - low)
        drain(SEND_Z, zr.at[:, away])
        for index, count_ in counts.items():
            if index in (SEND_V, SEND_SHARED):
                drain(index, vb.at[pl.ds(0, count_)])
            elif index == SEND_O:
                drain(index, ub.at[pl.ds(0, count_), pl.ds(0, low)])
            else:
                drain(index, ub.at[pl.ds(0, count_), pl.ds(low, half - low)])

    @pl.when(is_inner)
    def _():
        body(INNER)

    @pl.when(jnp.logical_not(is_inner))
    def _():
        body(OUTER)

    def meet(index, ref):
        pltpu.make_async_copy(ref, ref, meet_sem.at[index]).wait()

    result = part[0]
    meet(1, red.at[pl.ds(1, slots - 1)])
    for slot in range(1, slots):
        result = result + red[slot]
    size_x, size_y = lax.axis_size("sx"), lax.axis_size("sy")
    count = size_x * size_y
    rank = coords["sx"] * size_y + coords["sy"]
    every[pl.ds(rank, 1)] = result[None]

    def flipped(axis, mask):
        where = coords[axis]
        for bit in range(mask.bit_length()):
            if (mask >> bit) & 1:
                where = where + (1 << bit) * (1 - 2 * bit_of((axis, bit)))
        return where

    def b_copy(other):
        return pltpu.make_async_remote_copy(
            src_ref=every.at[rank],
            dst_ref=every.at[rank],
            send_sem=meet_sem.at[2],
            recv_sem=meet_sem.at[3],
            device_id=other,
            device_id_type=MESH,
        )

    if count <= 32:
        across_x = [flipped("sx", mask) for mask in range(size_x)]
        across_y = [flipped("sy", mask) for mask in range(size_y)]
        for mask in reversed(range(1, count)):
            b_copy((across_x[mask // size_y], across_y[mask % size_y])).start()
    else:

        @pl.loop(1, count)
        def _(offset):
            other = (rank + offset) % count
            b_copy((other // size_y, other % size_y)).start()

    meet(0, part.at[pl.ds(1, slots - 1)])
    meet(2, every.at[pl.ds(1, count - 1)])
    meet(3, every.at[pl.ds(1, count - 1)])

    if len(out_ref.shape) == 2:
        for index in range(count):
            out_ref[:, index * amps : (index + 1) * amps] = every[index]
    else:
        out_ref[0] = every[:, 0, :]
        out_ref[1] = every[:, 1, :]


def local(tensors, gates, closing_rows, closing_columns):
    current = tensors[:, 0, 0]
    rows, width = current.shape[1:]
    amps = closing_rows.shape[1]
    half = rows // 2
    bits_x = lax.axis_size("sx").bit_length() - 1
    bits_y = lax.axis_size("sy").bit_length() - 1
    exchanges = [(("sx", pos), pos) for pos in range(bits_x - 2)]
    gathers = [(("sy", pos), bits_x + pos) for pos in range(bits_y - 1)]
    plan = (exchanges, ("sx", bits_x - 2), ("sx", bits_x - 1), ("sy", bits_y - 1), gathers)
    stages, steps = len(exchanges), len(gathers)
    slots = 8 << steps
    count = lax.axis_size("sx") * lax.axis_size("sy")
    chunks = len(row_chunks(half))
    shape = (2, count * amps) if amps % 128 == 0 else (2, count, amps)
    grant = 55100 * 2**10 if amps % 128 == 0 else 62 * 2**20
    closed = pl.pallas_call(
        functools.partial(kernel, plan),
        out_shape=jax.ShapeDtypeStruct(shape, jnp.float32),
        in_specs=[pl.BlockSpec(memory_space=pl.ANY)] * 4,
        out_specs=pl.BlockSpec(memory_space=pltpu.VMEM),
        scratch_shapes=[
            pltpu.VMEM((stages + 1, 2, half, 2 * width), jnp.bfloat16),
            pltpu.VMEM((half, 2 * width), jnp.bfloat16),
            pltpu.VMEM((stages, 2, half, 2 * width), jnp.bfloat16),
            pltpu.VMEM((2, half, 2 * width), jnp.bfloat16),
            pltpu.VMEM((2, half, 4 * width), jnp.bfloat16),
            pltpu.VMEM((2, 2, amps, half), jnp.bfloat16),
            pltpu.VMEM((half, 2 * amps), jnp.bfloat16),
            pltpu.VMEM((slots, half, 2 * amps), jnp.bfloat16),
            pltpu.VMEM((2, amps, width), jnp.float32),
            pltpu.VMEM((slots, 2 * width, amps), jnp.bfloat16),
            pltpu.VMEM(gates.shape, jnp.bfloat16),
            pltpu.VMEM((stages, 4 * width, 2 * width), jnp.bfloat16),
            pltpu.VMEM((4 * width, 4 * width), jnp.bfloat16),
            pltpu.VMEM((2 + steps, 2, 2 * width, 2 * width), jnp.bfloat16),
            pltpu.VMEM((slots, 4 * width, 2 * amps), jnp.bfloat16),
            pltpu.VMEM((slots, 2, amps), jnp.float32),
            pltpu.VMEM((slots, 2, amps), jnp.float32),
            pltpu.VMEM((count, 2, amps), jnp.float32),
            pltpu.SemaphoreType.DMA((6,)),
            pltpu.SemaphoreType.DMA((7 + stages,)),
            pltpu.SemaphoreType.DMA((chunks,)),
            pltpu.SemaphoreType.DMA((stages, 2, chunks)),
            pltpu.SemaphoreType.DMA((2, chunks)),
            pltpu.SemaphoreType.DMA((2 * slots + 5,)),
            pltpu.SemaphoreType.DMA((4,)),
        ],
        compiler_params=pltpu.CompilerParams(
            collective_id=0, has_side_effects=True, vmem_limit_bytes=grant
        ),
    )(current, gates, closing_rows, closing_columns)
    return closed.reshape(2, count * amps)


def solution(mesh):
    placed = (
        P(None, "sx", "sy", None, None),
        P(),
        P(None, ("sx", "sy"), None),
        P(None, ("sx", "sy"), None),
    )
    return jax.shard_map(local, mesh=mesh, in_specs=placed, out_specs=P(), check_vma=False)
```
